32 devices in a mesh: groups: 2 (over y), ctx: 4 (over z), role: 2 (over x), seq: 2 (over core).
Axes of the slice: x: 2, y: 2, z: 4, core: 2. Of those that a mesh axis runs over, the one named last changes fastest.
Arguments:
- queries: bfloat16 [32, 128, 576], P(('groups', 'role', 'seq'), 'ctx'), parts along dimension 0, may hold values from -24 to 24
- cache: bfloat16 [16, 4096, 576], P(('groups', 'role', 'seq'), 'ctx'), parts along dimension 0, may hold values from -4 to 4
- lengths: int32 [16], P(('groups', 'role', 'seq')), parts along dimension 0, may hold values from 4 to 4096, as said below
- positions: int32 [32], P(('groups', 'role', 'seq')), parts along dimension 0, may hold values from 0 to 4098, as said below
- value_up_weight: bfloat16 [128, 512, 128], P('ctx', ('role', 'seq')), may hold values from -0.25 to 0.25
- out_proj: bfloat16 [16384, 7168], P('ctx', ('role', 'seq')), may hold values from -0.046875 to 0.046875
- residual: bfloat16 [32, 7168], P('groups', ('role', 'seq')), parts along dimension 0, may hold values from -4 to 4
- norm_gain: float32 [7168], P(('role', 'seq')), may hold values from 0.5 to 1.5
- gate_weight: bfloat16 [7168, 9216], P(('role', 'seq'), 'ctx'), may hold values from -0.0625 to 0.0625
- up_weight: bfloat16 [7168, 9216], P(('role', 'seq'), 'ctx'), may hold values from -0.0625 to 0.0625
- down_weight: bfloat16 [9216, 7168], P('ctx', ('role', 'seq')), may hold values from -0.0625 to 0.0625
Outputs:
- layer_out: bfloat16 [32, 7168], P(('groups', 'ctx'), ('role', 'seq')), parts along dimension 0
The draws below stay inside these ranges and needn't reach their ends.
There are 2 independent parts, one for each index of `groups`. The reference program is written for one: setup_inputs(seed, part) draws one part's arguments, and reference() takes and returns one part's arrays. A program takes and returns all parts, laid end to end along the dimension named above; an argument that names none is the same for every part. Nothing has to cross between parts.
Inputs may be any that keep to these rules, and one draw needn't show every extreme that they name: `lengths`: every sequence has at least 4 cached positions, and in every draw some sequence has all 4096. positions[r] lies between lengths[r // 2] - 4 and lengths[r // 2] + 2.
All inputs are finite; a program needn't handle non-finite values.
Results may differ from the reference program's by a relative error of at most 0.013.
Values may be sent and summed in bfloat16 or wider, within the bound.
A program may use at most 128 MiB of HBM per device.

```python
import jax
import jax.numpy as jnp
from jax import lax

D = 7168
HEADS = 128
LATENT = 512
ROPE = 64
VDIM = 128
FF = 9216
MTP = 2
CTX_DEV = 1024
SEQS = 8
ROWS = 16
CTX_LEN = 4096
N_CTX = 4


def length_table(key):
    base = jax.random.fold_in(key, 101)
    first_key, second_key = jax.random.split(base)
    spread = jax.random.randint(first_key, (SEQS,), 0, 1024)
    counts = 4 + spread * spread // 1024 * (CTX_LEN - 4) // 1024
    chosen = jax.random.randint(second_key, (), 0, SEQS)
    counts = jnp.where(jnp.arange(SEQS) == chosen, CTX_LEN, counts)
    return counts.astype(jnp.int32)


def draw_lengths(key, part):
    return length_table(key)


def draw_positions(key, part):
    counts = jnp.repeat(length_table(key), MTP)
    offsets = jax.random.randint(jax.random.fold_in(key, 102), (ROWS,), -4, 3)
    return (counts + offsets).astype(jnp.int32)


def draw_cache(key, part):
    value_vectors = jax.random.truncated_normal(jax.random.fold_in(key, 202), -4.0, 4.0, (SEQS, CTX_LEN, LATENT + ROPE), jnp.float32)
    return value_vectors.astype(jnp.bfloat16)


def draw_queries(key, part):
    value_vectors = jax.random.truncated_normal(jax.random.fold_in(key, 204), -4.0, 4.0, (ROWS, HEADS, LATENT + ROPE), jnp.float32)
    return value_vectors.astype(jnp.bfloat16)


def levels(own_key, shape, cuts, smallest, top_value):
    loudness = 1.0
    for position, blocks in cuts:
        heights = jax.random.uniform(jax.random.fold_in(jax.random.fold_in(own_key, 6), position), (blocks,), jnp.float32, smallest / len(cuts), top_value / len(cuts))
        loudness = loudness * jnp.repeat(jnp.exp(heights), shape[position] // blocks).reshape((-1,) + (1,) * (len(shape) - 1 - position))
    return loudness


def normal_values(key, dims, scale, limit, cuts=(), held_as=jnp.bfloat16):
    entries = jax.random.normal(key, dims, jnp.float32) * scale
    if len(cuts) > 0:
        entries = levels(key, dims, cuts, -0.22, 0.18) * entries
    return jnp.clip(entries, min=-limit, max=limit).astype(held_as)


def setup_inputs(seed: int = 0, part: int = 0) -> dict:
    keys = jax.random.split(jax.random.key(seed), 12)
    part_keys = jax.random.split(jax.random.fold_in(keys[11], part), 12)
    return {
        "queries": draw_queries(jax.random.fold_in(jax.random.fold_in(keys[11], part), 71), part),
        "cache": draw_cache(jax.random.fold_in(jax.random.fold_in(keys[11], part), 71), part),
        "lengths": draw_lengths(jax.random.fold_in(jax.random.fold_in(keys[11], part), 71), part),
        "positions": draw_positions(jax.random.fold_in(jax.random.fold_in(keys[11], part), 71), part),
        "value_up_weight": normal_values(keys[4], (HEADS, LATENT, VDIM), LATENT ** -0.5, 0.25, ((0, 4), (1, 4))),
        "out_proj": normal_values(keys[5], (HEADS * VDIM, D), (HEADS * VDIM) ** -0.5, 0.046875, ((0, 4), (1, 4))),
        "residual": normal_values(part_keys[6], (ROWS, D), 0.25, 4.0, ((1, 4),)),
        "norm_gain": jnp.clip(1.0 + 0.1 * jax.random.normal(keys[7], (D,), jnp.float32), 0.5, 1.5),
        "gate_weight": normal_values(keys[8], (D, FF), D ** -0.5, 0.0625, ((0, 4), (1, 4))),
        "up_weight": normal_values(keys[9], (D, FF), D ** -0.5, 0.0625, ((0, 4), (1, 4))),
        "down_weight": normal_values(keys[10], (FF, D), FF ** -0.5, 0.0625, ((0, 4), (1, 4))),
    }


softmax_scale = 0.07216878364870323
epsilon = 1e-06

def attend_single_sequence(packed):
    rows_pair, keys_all, length, spots = packed
    width = LATENT + ROPE
    flat_rows = rows_pair.reshape(MTP * HEADS, width)
    scores = jnp.dot(flat_rows, keys_all.T, preferred_element_type=jnp.float32) * softmax_scale
    places = jnp.arange(CTX_LEN, dtype=jnp.int32)
    limits = jnp.repeat(spots, HEADS)
    live = (places[None, :] < length) & (places[None, :] <= limits[:, None])
    scores = scores.reshape(MTP * HEADS, N_CTX, CTX_DEV)
    live = live.reshape(MTP * HEADS, N_CTX, CTX_DEV)
    block_max = lax.optimization_barrier(jnp.max(jnp.where(live, scores, jnp.float32(-1e+30)), axis=-1))
    probs = jnp.exp(jnp.where(live, scores - block_max[..., None], jnp.float32(-1e+30))).astype(jnp.bfloat16)
    block_weight_sum = lax.optimization_barrier(jnp.sum(probs.astype(jnp.float32), axis=-1))
    latents = keys_all[:, :LATENT].reshape(N_CTX, CTX_DEV, LATENT)
    block_out = jnp.einsum('hbj,bjd->hbd', probs.astype(jnp.float32), latents.astype(jnp.float32))
    highest = lax.optimization_barrier(jnp.max(block_max, axis=-1))
    factor = jnp.exp(block_max - highest[:, None])
    numer = lax.optimization_barrier(jnp.sum(factor[..., None] * block_out, axis=1))
    denom = lax.optimization_barrier(jnp.sum(factor * block_weight_sum, axis=1))
    return (numer / denom[:, None]).reshape(MTP, HEADS, LATENT)

def reference(queries, cache, lengths, positions, value_up_weight, out_proj, residual, norm_gain, gate_weight, up_weight, down_weight):
    grouped = queries.reshape(SEQS, MTP, HEADS, LATENT + ROPE)
    spots = positions.reshape(SEQS, MTP)
    attended_values = lax.map(attend_single_sequence, (grouped, cache, lengths, spots))
    attended_values = attended_values.reshape(ROWS, HEADS, LATENT).astype(jnp.bfloat16)
    value_vectors = jnp.einsum('nut,utc->nuc', attended_values.astype(jnp.float32), value_up_weight.astype(jnp.float32))
    value_vectors = value_vectors.astype(jnp.bfloat16).reshape(ROWS, HEADS * VDIM)
    attn_out = jnp.dot(value_vectors, out_proj, preferred_element_type=jnp.float32)
    resid = residual.astype(jnp.float32) + attn_out
    sumsq = lax.optimization_barrier(jnp.sum(resid * resid, axis=1))
    normed = (resid * lax.rsqrt(sumsq / D + epsilon)[:, None] * norm_gain[None, :]).astype(jnp.bfloat16)
    gate = jnp.dot(normed, gate_weight, preferred_element_type=jnp.float32)
    up = jnp.dot(normed, up_weight, preferred_element_type=jnp.float32)
    hidden = (jax.nn.silu(gate) * up).astype(jnp.bfloat16)
    return (resid + jnp.dot(hidden, down_weight, preferred_element_type=jnp.float32)).astype(jnp.bfloat16)
```

```python
import functools

import jax
import jax.numpy as jnp
from jax import lax
from jax.experimental import pallas as pl
from jax.experimental.pallas import tpu as pltpu
from jax.sharding import PartitionSpec as P

D = 7168
LATENT = 512
MTP = 2

softmax_scale = 0.07216878364870323
epsilon = 1e-06
MESH = pl.DeviceIdType.MESH
VMEM_BYTES = 60 * 1024 * 1024
f32, bf16 = jnp.float32, jnp.bfloat16


def ctx_group(n):
    me = lax.axis_index("ctx")

    def peer(d):
        k = lax.rem(me + d, n)
        return k, {"ctx": k}

    return me, peer


def feature_group(n_role, n_seq):
    n = n_role * n_seq
    me = lax.axis_index("role") * n_seq + lax.axis_index("seq")

    def peer(d):
        k = lax.rem(me + d, n)
        return k, {"role": k // n_seq, "seq": lax.rem(k, n_seq)}

    return me, peer


def enter(groups):
    barrier = pltpu.get_barrier_semaphore()
    count = 0
    for n, peer in groups:
        for d in range(1, n):
            pl.semaphore_signal(barrier, inc=1, device_id=peer(d)[1], device_id_type=MESH)
            count += 1
    pl.semaphore_wait(barrier, count)


def remote(src, dst, send, recv, device):
    return pltpu.make_async_remote_copy(
        src_ref=src, dst_ref=dst, send_sem=send, recv_sem=recv,
        device_id=device, device_id_type=MESH,
    )


def attend_kernel(n, n_role, n_seq, q_ref, cache_ref, len_ref, pos_ref, out_ref,
                  q_all, o_send, o_recv, s_send, s_recv, a_send, sems):
    nr = n_role * n_seq
    me, peer = ctx_group(n)
    fme, fpeer = feature_group(n_role, n_seq)
    enter(((n, peer), (nr, fpeer)))
    seqs, context, _ = cache_ref.shape
    rows = q_ref.shape[0] // seqs
    heads = rows // MTP

    q_copies = []
    for d in range(1, n):
        c = remote(q_ref, q_all.at[me], sems.at[0, d], sems.at[1, d], peer(d)[1])
        c.start()
        q_copies.append(c)

    places = me * context + lax.broadcasted_iota(jnp.int32, (rows, context), 1)
    first = lax.broadcasted_iota(jnp.int32, (rows, context), 0) < heads
    lives = []
    for s in range(seqs):
        limit = jnp.where(first, pos_ref[MTP * s], pos_ref[MTP * s + 1])
        lives.append((places < len_ref[s]) & (places <= limit))

    def block(q):
        outs, stats = [], []
        for s in range(seqs):
            keys = cache_ref[s]
            scores = lax.dot_general(
                q[s * rows:(s + 1) * rows], keys, (((1,), (1,)), ((), ())),
                preferred_element_type=f32) * softmax_scale
            live = lives[s]
            top = jnp.max(jnp.where(live, scores, -1e30), axis=1, keepdims=True)
            probs = jnp.exp(jnp.where(live, scores - top, -1e30)).astype(bf16)
            total = jnp.sum(probs.astype(f32), axis=1, keepdims=True)
            outs.append(jnp.dot(probs, keys[:, :LATENT], preferred_element_type=f32))
            lane = lax.broadcasted_iota(jnp.int32, (rows, 128), 1)
            stats.append(jnp.where(lane == 0, top, total))
        return jnp.concatenate(outs, axis=0), jnp.concatenate(stats, axis=0)

    own_o, own_s = block(q_ref[...])
    o_copies, s_copies = [], []
    for d in range(1, n):
        src, device = peer(n - d)
        remote(q_all.at[src], q_all.at[src], sems.at[0, d], sems.at[1, d], device).wait_recv()
        o, s = block(q_all[src])
        o_send[d] = o.astype(bf16)
        s_send[d] = s.T[0:8]
        c = remote(o_send.at[d], o_recv.at[d], sems.at[2, d], sems.at[3, d], device)
        c.start()
        o_copies.append(c)
        c = remote(s_send.at[d], s_recv.at[d], sems.at[4, d], sems.at[5, d], device)
        c.start()
        s_copies.append(c)
    for c in q_copies:
        c.wait_send()

    all_rows = q_ref.shape[0]
    tops, totals = [own_s[:, 0:1]], [own_s[:, 1:2]]
    for d in range(1, n):
        s_copies[d - 1].wait()
        back = jnp.concatenate([s_recv[d]] * 16, axis=0).T
        tops.append(back[:, 0:1])
        totals.append(back[:, 1:2])
    highest = functools.reduce(jnp.maximum, tops)
    factors = [jnp.exp(t - highest) for t in tops]
    denom = sum(f * t for f, t in zip(factors, totals))
    numer = factors[0] * own_o
    for d in range(1, n):
        o_copies[d - 1].wait()
        numer = numer + factors[d] * o_recv[d].astype(f32)
    attended = (numer / denom).astype(bf16)

    part = LATENT // nr
    for k in range(nr):
        a_send[k] = attended[:, k * part:(k + 1) * part]
    copies = []
    for d in range(1, nr):
        k, device = fpeer(d)
        c = remote(a_send.at[k], out_ref.at[fme], sems.at[6, d], sems.at[7, d], device)
        c.start()
        copies.append(c)
    out_ref[fme] = a_send[fme]
    for d in range(1, nr):
        k, device = fpeer(nr - d)
        copies[d - 1].wait_send()
        remote(a_send.at[k], out_ref.at[k], sems.at[6, d], sems.at[7, d], device).wait_recv()


def layer_kernel(n, n_role, n_seq, pv_ref, res_ref, gain_ref, wo_hbm, wg_hbm, wu_hbm, wd_hbm,
                 out_ref, wo, wg, wu, wd, pv_recv, v_send, v_all, v_full, acc, po_send, po_recv,
                 resid, xg_ref, g_acc, u_acc, gu_send, gu_recv, ss_send, ss_recv, h_send, h_all,
                 h_full, dn, dn_send, dn_recv, wsem, sems):
    nr = n_role * n_seq
    me, peer = ctx_group(n)
    fme, fpeer = feature_group(n_role, n_seq)

    weights = []
    for which, (hbm, vmem) in enumerate(((wo_hbm, wo), (wg_hbm, wg), (wu_hbm, wu), (wd_hbm, wd))):
        depth = vmem.shape[1]

        def fetch(i, hbm=hbm, vmem=vmem, depth=depth, which=which):
            return pltpu.make_async_copy(
                hbm.at[pl.ds(i * depth, depth)], vmem.at[i], wsem.at[which, i])

        weights.append((fetch, vmem))
    for fetch, vmem in weights:
        for i in range(vmem.shape[0]):
            fetch(i).start()
    enter(((n, peer), (nr, fpeer)))

    def matmul(x_ref, which, acc_ref):
        fetch, vmem = weights[which]
        depth = vmem.shape[1]
        acc_ref[...] = jnp.zeros_like(acc_ref)
        if vmem.shape[0] == 1:
            fetch(0).wait()
            acc_ref[...] = jnp.dot(x_ref[...], vmem[0], preferred_element_type=f32)
            return

        @pl.loop(0, vmem.shape[0])
        def _(i):
            fetch(i).wait()
            x = x_ref[:, pl.ds(pl.multiple_of(i * depth, depth), depth)]
            acc_ref[...] += jnp.dot(x, vmem[i], preferred_element_type=f32)

    def swap(size, peer_of, chunk, recv, row):
        copies = []
        for d in range(1, size):
            k, device = peer_of(d)
            c = remote(chunk(k), recv.at[d], sems.at[row, d], sems.at[row + 1, d], device)
            c.start()
            copies.append(c)
        return copies

    def gather(size, my, peer_of, send, full, row):
        copies = []
        for d in range(1, size):
            c = remote(send, full.at[my], sems.at[row, d], sems.at[row + 1, d], peer_of(d)[1])
            c.start()
            copies.append(c)
        full[my] = send[...]
        for d in range(1, size):
            k, device = peer_of(size - d)
            copies[d - 1].wait_send()
            remote(send, full.at[k], sems.at[row, d], sems.at[row + 1, d], device).wait_recv()

    part = res_ref.shape[0] // nr
    copies = swap(nr, fpeer, lambda k: pv_ref.at[k], pv_recv, 0)
    vals = pv_ref[fme].astype(f32)
    for d in range(1, nr):
        copies[d - 1].wait()
        vals = vals + pv_recv[d].astype(f32)
    v_send[...] = vals.astype(bf16)
    gather(nr, fme, fpeer, v_send, v_all, 2)
    for k in range(nr):
        acc_rows = v_all[k].astype(f32)
        v_full[k * part:(k + 1) * part, :] = acc_rows
    x_ref = xg_ref[0]
    x_ref[...] = v_full[...].astype(bf16)
    matmul(x_ref, 0, acc)

    po_send[...] = acc[...].astype(bf16)
    copies = swap(n, peer, lambda k: po_send, po_recv, 4)
    total = res_ref[...].astype(f32) + acc[...]
    for d in range(1, n):
        copies[d - 1].wait()
        total = total + po_recv[d].astype(f32)
    crows = res_ref.shape[0] // n
    for k in range(n):
        resid[k] = total[k * crows:(k + 1) * crows]
    sumsq = jnp.sum(total * total, axis=1, keepdims=True)
    sumsq = jnp.broadcast_to(sumsq, (total.shape[0], 128))
    for k in range(nr):
        ss_send[k] = sumsq[k * part:(k + 1) * part]
    s_copies = swap(nr, fpeer, lambda k: ss_send.at[k], ss_recv, 6)
    x_ref = xg_ref[1]
    x_ref[...] = (total * gain_ref[...]).astype(bf16)
    matmul(x_ref, 1, g_acc)
    matmul(x_ref, 2, u_acc)

    for j, a in enumerate((g_acc, u_acc)):
        for k in range(nr):
            gu_send[k, j] = a[k * part:(k + 1) * part, :].astype(bf16)
    copies = swap(nr, fpeer, lambda k: gu_send.at[k], gu_recv, 8)
    ss = ss_send[fme]
    for d in range(1, nr):
        s_copies[d - 1].wait()
        ss = ss + ss_recv[d]
    inv = lax.rsqrt(ss[:, 0:1] / D + epsilon)
    gate = gu_send[fme, 0].astype(f32)
    up = gu_send[fme, 1].astype(f32)
    for d in range(1, nr):
        copies[d - 1].wait()
        gate = gate + gu_recv[d, 0].astype(f32)
        up = up + gu_recv[d, 1].astype(f32)
    gate = gate * inv
    up = up * inv
    h_send[...] = (gate / (1.0 + jnp.exp(-gate)) * up).astype(bf16)
    gather(nr, fme, fpeer, h_send, h_all, 10)
    for k in range(nr):
        h_full[k * part:(k + 1) * part, :] = h_all[k].astype(f32)
    x_ref = xg_ref[2]
    x_ref[...] = h_full[...].astype(bf16)
    matmul(x_ref, 3, acc)

    for k in range(n):
        piece = acc[k * crows:(k + 1) * crows, :]
        dn[k] = piece
        dn_send[k] = piece.astype(bf16)
    copies = swap(n, peer, lambda k: dn_send.at[k], dn_recv, 12)
    result = resid[me] + dn[me]
    for d in range(1, n):
        copies[d - 1].wait()
        result = result + dn_recv[d].astype(f32)
    out_ref[...] = result.astype(bf16)


def chunk_of(depth):
    for size in (512, 256):
        if depth % size == 0:
            return size
    return depth


def per_device(sizes, queries, cache, lengths, positions, value_up_weight, out_proj, residual,
               norm_gain, gate_weight, up_weight, down_weight):
    n, n_role, n_seq = sizes
    nr = n_role * n_seq
    rows, heads, width = queries.shape
    flat = rows * heads
    lat = LATENT // nr
    vmem = pl.BlockSpec(memory_space=pltpu.VMEM)
    smem = pl.BlockSpec(memory_space=pltpu.SMEM)
    hbm = pl.BlockSpec(memory_space=pl.ANY)
    most = max(n, nr)
    sems = lambda k: pltpu.SemaphoreType.DMA((k, most))
    attended = pl.pallas_call(
        functools.partial(attend_kernel, n, n_role, n_seq),
        out_shape=jax.ShapeDtypeStruct((nr, flat, lat), bf16),
        in_specs=[vmem, vmem, smem, smem],
        out_specs=vmem,
        scratch_shapes=[
            pltpu.VMEM((n, flat, width), bf16),
            pltpu.VMEM((n, flat, LATENT), bf16),
            pltpu.VMEM((n, flat, LATENT), bf16),
            pltpu.VMEM((n, 8, flat), f32),
            pltpu.VMEM((n, 8, flat), f32),
            pltpu.VMEM((nr, flat, lat), bf16),
            sems(8),
        ],
        compiler_params=pltpu.CompilerParams(
            collective_id=0, has_side_effects=True, vmem_limit_bytes=VMEM_BYTES),
        name="attend",
    )(queries.reshape(flat, width), cache, lengths, positions)
    by_head = attended.reshape(nr, rows, heads, lat).transpose(2, 0, 1, 3).reshape(heads, nr * rows, lat)
    mixed = jnp.einsum("hrk,hkv->rhv", by_head, value_up_weight, preferred_element_type=f32)
    vwide = heads * value_up_weight.shape[2]
    pv = mixed.astype(bf16).reshape(nr, rows, vwide)

    all_rows, dd = residual.shape
    ff = gate_weight.shape[1]
    part, crows = all_rows // nr, all_rows // n

    def held(w):
        size = chunk_of(w.shape[0])
        return pltpu.VMEM((w.shape[0] // size, size, w.shape[1]), bf16)

    ws = (out_proj, gate_weight, up_weight, down_weight)
    most_chunks = max(w.shape[0] // chunk_of(w.shape[0]) for w in ws)
    V = pltpu.VMEM
    return pl.pallas_call(
        functools.partial(layer_kernel, n, n_role, n_seq),
        out_shape=jax.ShapeDtypeStruct((crows, dd), bf16),
        in_specs=[vmem] * 3 + [hbm] * 4,
        out_specs=vmem,
        scratch_shapes=[
            *[held(w) for w in ws],
            V((nr, part, vwide), bf16),
            V((part, vwide), bf16),
            V((nr, part, vwide), bf16),
            V((all_rows, vwide), f32),
            V((all_rows, dd), f32),
            V((all_rows, dd), bf16),
            V((n, all_rows, dd), bf16),
            V((n, crows, dd), f32),
            [V((all_rows, vwide), bf16), V((all_rows, dd), bf16), V((all_rows, ff), bf16)],
            V((all_rows, ff), f32),
            V((all_rows, ff), f32),
            V((nr, 2, part, ff), bf16),
            V((nr, 2, part, ff), bf16),
            V((nr, part, 128), f32),
            V((nr, part, 128), f32),
            V((part, ff), bf16),
            V((nr, part, ff), bf16),
            V((all_rows, ff), f32),
            V((n, crows, dd), f32),
            V((n, crows, dd), bf16),
            V((n, crows, dd), bf16),
            pltpu.SemaphoreType.DMA((4, most_chunks)),
            sems(14),
        ],
        compiler_params=pltpu.CompilerParams(
            collective_id=1, has_side_effects=True, vmem_limit_bytes=VMEM_BYTES),
        name="layer",
    )(pv, residual, norm_gain.reshape(1, dd), *ws)


def solution(mesh):
    placed = (
        P(("groups", "role", "seq"), "ctx", None),
        P(("groups", "role", "seq"), "ctx", None),
        P(("groups", "role", "seq")),
        P(("groups", "role", "seq")),
        P("ctx", ("role", "seq"), None),
        P("ctx", ("role", "seq")),
        P("groups", ("role", "seq")),
        P(("role", "seq")),
        P(("role", "seq"), "ctx"),
        P(("role", "seq"), "ctx"),
        P("ctx", ("role", "seq")),
    )
    sizes = (mesh.shape["ctx"], mesh.shape["role"], mesh.shape["seq"])
    return jax.shard_map(
        functools.partial(per_device, sizes),
        mesh=mesh,
        in_specs=placed,
        out_specs=P(("groups", "ctx"), ("role", "seq")),
        check_vma=False,
    )
```

```python
import functools

import jax
import jax.numpy as jnp
from jax import lax
from jax.experimental import pallas as pl
from jax.experimental.pallas import tpu as pltpu
from jax.sharding import PartitionSpec as P

D = 7168
LATENT = 512
MTP = 2

softmax_scale = 0.07216878364870323
epsilon = 1e-06
MESH = pl.DeviceIdType.MESH
VMEM_BYTES = 60 * 1024 * 1024
f32, bf16 = jnp.float32, jnp.bfloat16


def ctx_group(n):
    me = lax.axis_index("ctx")

    def peer(d):
        k = lax.rem(me + d, n)
        return k, {"ctx": k}

    return me, peer


def feature_group(n_role, n_seq):
    n = n_role * n_seq
    me = lax.axis_index("role") * n_seq + lax.axis_index("seq")

    def peer(d):
        k = lax.rem(me + d, n)
        return k, {"role": k // n_seq, "seq": lax.rem(k, n_seq)}

    return me, peer


def enter(groups):
    barrier = pltpu.get_barrier_semaphore()
    count = 0
    for n, peer in groups:
        for d in range(1, n):
            pl.semaphore_signal(barrier, inc=1, device_id=peer(d)[1], device_id_type=MESH)
            count += 1
    pl.semaphore_wait(barrier, count)


def remote(src, dst, send, recv, device):
    return pltpu.make_async_remote_copy(
        src_ref=src, dst_ref=dst, send_sem=send, recv_sem=recv,
        device_id=device, device_id_type=MESH,
    )


def attend(n, n_role, n_seq, q_ref, cache_ref, cache_copy, len_ref, pos_ref, out_ref,
           q_all, o_send, o_recv, s_send, s_recv, a_send, sems):
    nr = n_role * n_seq
    me, peer = ctx_group(n)
    fme, fpeer = feature_group(n_role, n_seq)
    seqs, _, context = cache_ref.shape
    rows = q_ref.shape[0] // seqs
    heads = rows // MTP

    q_copies = []
    for d in range(1, n):
        c = remote(q_ref, q_all.at[me], sems.at[0, d], sems.at[1, d], peer(d)[1])
        c.start()
        q_copies.append(c)

    places = me * context + lax.broadcasted_iota(jnp.int32, (rows, context), 1)
    first = lax.broadcasted_iota(jnp.int32, (rows, context), 0) < heads
    lives = []
    for s in range(seqs):
        limit = jnp.where(first, pos_ref[MTP * s], pos_ref[MTP * s + 1])
        lives.append((places < len_ref[s]) & (places <= limit))

    def block(q):
        outs, stats = [], []
        for s in range(seqs):
            keys = cache_ref[s]
            scores = lax.dot_general(
                q[s * rows:(s + 1) * rows], keys, (((1,), (0,)), ((), ())),
                preferred_element_type=f32) * softmax_scale
            live = lives[s]
            top = jnp.max(jnp.where(live, scores, -1e30), axis=1, keepdims=True)
            probs = jnp.exp(jnp.where(live, scores - top, -1e30)).astype(bf16)
            total = jnp.sum(probs.astype(f32), axis=1, keepdims=True)
            outs.append(lax.dot_general(
                probs, keys[:LATENT], (((1,), (1,)), ((), ())), preferred_element_type=f32))
            lane = lax.broadcasted_iota(jnp.int32, (rows, 128), 1)
            stats.append(jnp.where(lane == 0, top, total))
        return jnp.concatenate(outs, axis=0), jnp.concatenate(stats, axis=0)

    cache_copy.wait()
    own_o, own_s = block(q_ref[...])
    o_copies, s_copies = [], []
    for d in range(1, n):
        src, device = peer(n - d)
        remote(q_all.at[src], q_all.at[src], sems.at[0, d], sems.at[1, d], device).wait_recv()
        o, s = block(q_all[src])
        o_send[d] = o.astype(bf16)
        s_send[d] = s.T[0:8]
        c = remote(o_send.at[d], o_recv.at[d], sems.at[2, d], sems.at[3, d], device)
        c.start()
        o_copies.append(c)
        c = remote(s_send.at[d], s_recv.at[d], sems.at[4, d], sems.at[5, d], device)
        c.start()
        s_copies.append(c)
    for c in q_copies:
        c.wait_send()

    all_rows = q_ref.shape[0]
    tops, totals = [own_s[:, 0:1]], [own_s[:, 1:2]]
    for d in range(1, n):
        s_copies[d - 1].wait()
        back = jnp.concatenate([s_recv[d]] * 16, axis=0).T
        tops.append(back[:, 0:1])
        totals.append(back[:, 1:2])
    highest = functools.reduce(jnp.maximum, tops)
    factors = [jnp.exp(t - highest) for t in tops]
    denom = sum(f * t for f, t in zip(factors, totals))
    numer = factors[0] * own_o
    for d in range(1, n):
        o_copies[d - 1].wait()
        numer = numer + factors[d] * o_recv[d].astype(f32)
    attended = (numer / denom).astype(bf16)

    part = LATENT // nr
    for k in range(nr):
        for r in range(all_rows // heads):
            a_send[k, r] = attended[r * heads:(r + 1) * heads, k * part:(k + 1) * part]
    copies = []
    for d in range(1, nr):
        k, device = fpeer(d)
        c = remote(a_send.at[k], out_ref.at[fme], sems.at[6, d], sems.at[7, d], device)
        c.start()
        copies.append(c)
    out_ref[fme] = a_send[fme]
    for d in range(1, nr):
        k, device = fpeer(nr - d)
        copies[d - 1].wait_send()
        remote(a_send.at[k], out_ref.at[k], sems.at[6, d], sems.at[7, d], device).wait_recv()


def layer_kernel(n, n_role, n_seq, q_ref, cache_hbm, len_ref, pos_ref, vu_hbm, res_ref, gain_ref,
                 wo_hbm, wg_hbm, wu_hbm, wd_hbm,
                 out_ref, cache, vu, q_all, o_send, o_recv, s_send, s_recv, a_send, a_all, a_head,
                 mixed, pv_ref, wo, wg, wu, wd, pv_recv, v_send, v_all, v_full, acc, po_send,
                 po_recv, resid, xg_ref, g_acc, u_acc, gu_send, gu_recv, ss_send, ss_recv, h_send,
                 h_all, h_full, dn, dn_send, dn_recv, wsem, lsem, asems, sems):
    nr = n_role * n_seq
    me, peer = ctx_group(n)
    fme, fpeer = feature_group(n_role, n_seq)

    cache_copy = pltpu.make_async_copy(cache_hbm, cache, lsem.at[0])
    cache_copy.start()
    vu_copy = pltpu.make_async_copy(vu_hbm, vu, lsem.at[1])
    vu_copy.start()
    weights = []
    for which, (hbm, vmem) in enumerate(((wo_hbm, wo), (wg_hbm, wg), (wu_hbm, wu), (wd_hbm, wd))):
        depth = vmem.shape[1]

        def fetch(i, hbm=hbm, vmem=vmem, depth=depth, which=which):
            return pltpu.make_async_copy(
                hbm.at[pl.ds(i * depth, depth)], vmem.at[i], wsem.at[which, i])

        weights.append((fetch, vmem))
    for fetch, vmem in weights:
        for i in range(vmem.shape[0]):
            fetch(i).start()
    enter(((n, peer), (nr, fpeer)))
    attend(n, n_role, n_seq, q_ref, cache, cache_copy, len_ref, pos_ref, a_all,
           q_all, o_send, o_recv, s_send, s_recv, a_send, asems)
    rows, heads = a_all.shape[1:3]
    for j in range(nr):
        for r in range(rows):
            a_head[:, j * rows + r, :] = a_all[j, r].astype(f32)
    vu_copy.wait()
    vdim = vu.shape[2]
    for h in range(heads):
        mixed[:, h * vdim:(h + 1) * vdim] = jnp.dot(
            a_head[h].astype(bf16), vu[h], preferred_element_type=f32)
    for k in range(nr):
        pv_ref[k] = mixed[k * rows:(k + 1) * rows, :].astype(bf16)

    def matmul(x_ref, *pairs):
        chunks, depth, _ = weights[pairs[0][0]][1].shape
        for which, acc_ref in pairs:
            fetch, vmem = weights[which]
            fetch(0).wait()
            acc_ref[...] = jnp.dot(x_ref[:, :depth], vmem[0], preferred_element_type=f32)
        if chunks == 1:
            return

        @pl.loop(1, chunks)
        def _(i):
            x = x_ref[:, pl.ds(pl.multiple_of(i * depth, depth), depth)]
            for which, acc_ref in pairs:
                fetch, vmem = weights[which]
                fetch(i).wait()
                acc_ref[...] += jnp.dot(x, vmem[i], preferred_element_type=f32)

    def swap(size, peer_of, chunk, recv, row):
        copies = []
        for d in range(1, size):
            k, device = peer_of(d)
            c = remote(chunk(k), recv.at[d], sems.at[row, d], sems.at[row + 1, d], device)
            c.start()
            copies.append(c)
        return copies

    def gather(size, my, peer_of, send, full, row):
        copies = []
        for d in range(1, size):
            c = remote(send, full.at[my], sems.at[row, d], sems.at[row + 1, d], peer_of(d)[1])
            c.start()
            copies.append(c)
        full[my] = send[...]
        for d in range(1, size):
            k, device = peer_of(size - d)
            copies[d - 1].wait_send()
            remote(send, full.at[k], sems.at[row, d], sems.at[row + 1, d], device).wait_recv()

    part = res_ref.shape[0] // nr
    copies = swap(nr, fpeer, lambda k: pv_ref.at[k], pv_recv, 0)
    vals = pv_ref[fme].astype(f32)
    for d in range(1, nr):
        copies[d - 1].wait()
        vals = vals + pv_recv[d].astype(f32)
    v_send[...] = vals.astype(bf16)
    gather(nr, fme, fpeer, v_send, v_all, 2)
    for k in range(nr):
        acc_rows = v_all[k].astype(f32)
        v_full[k * part:(k + 1) * part, :] = acc_rows
    x_ref = xg_ref[0]
    x_ref[...] = v_full[...].astype(bf16)
    matmul(x_ref, (0, acc))

    po_send[...] = acc[...].astype(bf16)
    copies = swap(n, peer, lambda k: po_send, po_recv, 4)
    total = res_ref[...].astype(f32) + acc[...]
    for d in range(1, n):
        copies[d - 1].wait()
        total = total + po_recv[d].astype(f32)
    crows = res_ref.shape[0] // n
    for k in range(n):
        resid[k] = total[k * crows:(k + 1) * crows]
    sumsq = jnp.sum(total * total, axis=1, keepdims=True)
    sumsq = jnp.broadcast_to(sumsq, (total.shape[0], 128))
    for k in range(nr):
        ss_send[k] = sumsq[k * part:(k + 1) * part]
    s_copies = swap(nr, fpeer, lambda k: ss_send.at[k], ss_recv, 6)
    x_ref = xg_ref[1]
    x_ref[...] = (total * gain_ref[...]).astype(bf16)
    matmul(x_ref, (1, g_acc), (2, u_acc))

    for j, a in enumerate((g_acc, u_acc)):
        for k in range(nr):
            gu_send[k, j] = a[k * part:(k + 1) * part, :].astype(bf16)
    copies = swap(nr, fpeer, lambda k: gu_send.at[k], gu_recv, 8)
    ss = ss_send[fme]
    for d in range(1, nr):
        s_copies[d - 1].wait()
        ss = ss + ss_recv[d]
    inv = lax.rsqrt(ss[:, 0:1] / D + epsilon)
    gate = gu_send[fme, 0].astype(f32)
    up = gu_send[fme, 1].astype(f32)
    for d in range(1, nr):
        copies[d - 1].wait()
        gate = gate + gu_recv[d, 0].astype(f32)
        up = up + gu_recv[d, 1].astype(f32)
    gate = gate * inv
    up = up * inv
    h_send[...] = (gate / (1.0 + jnp.exp(-gate)) * up).astype(bf16)
    gather(nr, fme, fpeer, h_send, h_all, 10)
    for k in range(nr):
        h_full[k * part:(k + 1) * part, :] = h_all[k].astype(f32)
    x_ref = xg_ref[2]
    x_ref[...] = h_full[...].astype(bf16)
    matmul(x_ref, (3, acc))

    for k in range(n):
        piece = acc[k * crows:(k + 1) * crows, :]
        dn[k] = piece
        dn_send[k] = piece.astype(bf16)
    copies = swap(n, peer, lambda k: dn_send.at[k], dn_recv, 12)
    result = resid[me] + dn[me]
    for d in range(1, n):
        copies[d - 1].wait()
        result = result + dn_recv[d].astype(f32)
    out_ref[...] = result.astype(bf16)


def chunk_of(depth):
    for size in (1024, 768, 512, 256):
        if depth % size == 0:
            return size
    return depth


def per_device(sizes, queries, cache, lengths, positions, value_up_weight, out_proj, residual,
               norm_gain, gate_weight, up_weight, down_weight):
    n, n_role, n_seq = sizes
    nr = n_role * n_seq
    rows, heads, width = queries.shape
    flat = rows * heads
    lat = LATENT // nr
    vmem = pl.BlockSpec(memory_space=pltpu.VMEM)
    smem = pl.BlockSpec(memory_space=pltpu.SMEM)
    hbm = pl.BlockSpec(memory_space=pl.ANY)
    most = max(n, nr)
    sems = lambda k: pltpu.SemaphoreType.DMA((k, most))
    vwide = heads * value_up_weight.shape[2]
    all_rows, dd = residual.shape
    ff = gate_weight.shape[1]
    part, crows = all_rows // nr, all_rows // n

    def held(w):
        size = chunk_of(w.shape[0])
        return pltpu.VMEM((w.shape[0] // size, size, w.shape[1]), bf16)

    ws = (out_proj, gate_weight, up_weight, down_weight)
    most_chunks = max(w.shape[0] // chunk_of(w.shape[0]) for w in ws)
    V = pltpu.VMEM
    return pl.pallas_call(
        functools.partial(layer_kernel, n, n_role, n_seq),
        out_shape=jax.ShapeDtypeStruct((crows, dd), bf16),
        in_specs=[vmem, hbm, smem, smem, hbm, vmem, vmem] + [hbm] * 4,
        out_specs=vmem,
        scratch_shapes=[
            V((cache.shape[0], width, cache.shape[1]), bf16),
            V(value_up_weight.shape, bf16),
            V((n, flat, width), bf16),
            V((n, flat, LATENT), bf16),
            V((n, flat, LATENT), bf16),
            V((n, 8, flat), f32),
            V((n, 8, flat), f32),
            V((nr, rows, heads, lat), bf16),
            V((nr, rows, heads, lat), bf16),
            V((heads, all_rows, lat), f32),
            V((all_rows, vwide), f32),
            V((nr, part, vwide), bf16),
            *[held(w) for w in ws],
            V((nr, part, vwide), bf16),
            V((part, vwide), bf16),
            V((nr, part, vwide), bf16),
            V((all_rows, vwide), f32),
            V((all_rows, dd), f32),
            V((all_rows, dd), bf16),
            V((n, all_rows, dd), bf16),
            V((n, crows, dd), f32),
            [V((all_rows, vwide), bf16), V((all_rows, dd), bf16), V((all_rows, ff), bf16)],
            V((all_rows, ff), f32),
            V((all_rows, ff), f32),
            V((nr, 2, part, ff), bf16),
            V((nr, 2, part, ff), bf16),
            V((nr, part, 128), f32),
            V((nr, part, 128), f32),
            V((part, ff), bf16),
            V((nr, part, ff), bf16),
            V((all_rows, ff), f32),
            V((n, crows, dd), f32),
            V((n, crows, dd), bf16),
            V((n, crows, dd), bf16),
            pltpu.SemaphoreType.DMA((4, most_chunks)),
            pltpu.SemaphoreType.DMA((2,)),
            sems(8),
            sems(14),
        ],
        compiler_params=pltpu.CompilerParams(
            collective_id=0, has_side_effects=True, vmem_limit_bytes=VMEM_BYTES),
        name="layer",
    )(queries.reshape(flat, width), cache.transpose(0, 2, 1), lengths, positions, value_up_weight,
      residual, norm_gain.reshape(1, dd), *ws)


def solution(mesh):
    placed = (
        P(("groups", "role", "seq"), "ctx", None),
        P(("groups", "role", "seq"), "ctx", None),
        P(("groups", "role", "seq")),
        P(("groups", "role", "seq")),
        P("ctx", ("role", "seq"), None),
        P("ctx", ("role", "seq")),
        P("groups", ("role", "seq")),
        P(("role", "seq")),
        P(("role", "seq"), "ctx"),
        P(("role", "seq"), "ctx"),
        P("ctx", ("role", "seq")),
    )
    sizes = (mesh.shape["ctx"], mesh.shape["role"], mesh.shape["seq"])
    return jax.shard_map(
        functools.partial(per_device, sizes),
        mesh=mesh,
        in_specs=placed,
        out_specs=P(("groups", "ctx"), ("role", "seq")),
        check_vma=False,
    )
```

```python
import functools

import jax
import jax.numpy as jnp
from jax import lax
from jax.experimental import pallas as pl
from jax.experimental.pallas import tpu as pltpu
from jax.sharding import PartitionSpec as P

D = 7168
LATENT = 512
MTP = 2

softmax_scale = 0.07216878364870323
epsilon = 1e-06
MESH = pl.DeviceIdType.MESH
VMEM_BYTES = 60 * 1024 * 1024
f32, bf16 = jnp.float32, jnp.bfloat16


def ctx_group(n):
    me = lax.axis_index("ctx")

    def peer(d):
        k = lax.rem(me + d, n)
        return k, {"ctx": k}

    return me, peer


def feature_group(n_role, n_seq):
    n = n_role * n_seq
    me = lax.axis_index("role") * n_seq + lax.axis_index("seq")

    def peer(d):
        k = lax.rem(me + d, n)
        return k, {"role": k // n_seq, "seq": lax.rem(k, n_seq)}

    return me, peer


def enter(groups):
    barrier = pltpu.get_barrier_semaphore()
    count = 0
    for n, peer in groups:
        for d in range(1, n):
            pl.semaphore_signal(barrier, inc=1, device_id=peer(d)[1], device_id_type=MESH)
            count += 1
    pl.semaphore_wait(barrier, count)


def remote(src, dst, send, recv, device):
    return pltpu.make_async_remote_copy(
        src_ref=src, dst_ref=dst, send_sem=send, recv_sem=recv,
        device_id=device, device_id_type=MESH,
    )


def attend(n, n_role, n_seq, q_ref, cache_ref, cache_copy, len_ref, pos_ref, out_ref,
           q_all, o_send, o_recv, s_send, s_recv, a_send, sems):
    nr = n_role * n_seq
    me, peer = ctx_group(n)
    fme, fpeer = feature_group(n_role, n_seq)
    seqs, _, context = cache_ref.shape
    rows = q_ref.shape[1]
    heads = rows // MTP

    q_copies = []
    for s in range(seqs):
        for d in range(1, n):
            c = remote(q_ref.at[s], q_all.at[me, s], sems.at[s, d], sems.at[seqs + s, d],
                       peer(d)[1])
            c.start()
            q_copies.append(c)

    places = me * context + lax.broadcasted_iota(jnp.int32, (rows, context), 1)
    first = lax.broadcasted_iota(jnp.int32, (rows, context), 0) < heads
    lives = []
    for s in range(seqs):
        limit = jnp.where(first, pos_ref[MTP * s], pos_ref[MTP * s + 1])
        lives.append((places < len_ref[s]) & (places <= limit))

    lane = lax.broadcasted_iota(jnp.int32, (rows, 128), 1)

    def block(q, s):
        keys = cache_ref[s]
        scores = jnp.dot(q, keys, preferred_element_type=f32) * softmax_scale
        live = lives[s]
        top = jnp.max(jnp.where(live, scores, -1e30), axis=1, keepdims=True)
        probs = jnp.exp(jnp.where(live, scores - top, -1e30)).astype(bf16)
        total = jnp.sum(probs.astype(f32), axis=1, keepdims=True)
        out = lax.dot_general(
            probs, keys[:LATENT], (((1,), (1,)), ((), ())), preferred_element_type=f32)
        return out, top, total

    cache_copy.wait()
    own = [block(q_ref[s], s) for s in range(seqs)]
    o_copies, s_copies = {}, {}
    for s in range(seqs):
        for d in range(1, n):
            src, device = peer(n - d)
            remote(q_ref.at[s], q_all.at[src, s], sems.at[s, d], sems.at[seqs + s, d],
                   device).wait_recv()
            o, top, total = block(q_all[src, s], s)
            o_send[d, s] = o.astype(bf16)
            s_send[d, s] = jnp.where(lane == 0, top, total).T[0:8]
            c = remote(o_send.at[d, s], o_recv.at[d, s], sems.at[2 * seqs + s, d],
                       sems.at[3 * seqs + s, d], device)
            c.start()
            o_copies[s, d] = c
            c = remote(s_send.at[d, s], s_recv.at[d, s], sems.at[4 * seqs + s, d],
                       sems.at[5 * seqs + s, d], device)
            c.start()
            s_copies[s, d] = c
    for c in q_copies:
        c.wait_send()

    heads = rows // MTP
    merged = []
    for s in range(seqs):
        own_o, top, total = own[s]
        tops, totals = [top], [total]
        for d in range(1, n):
            s_copies[s, d].wait()
            back = jnp.concatenate([s_recv[d, s]] * 16, axis=0).T
            tops.append(back[:, 0:1])
            totals.append(back[:, 1:2])
        highest = functools.reduce(jnp.maximum, tops)
        factors = [jnp.exp(t - highest) for t in tops]
        denom = sum(f * t for f, t in zip(factors, totals))
        numer = factors[0] * own_o
        for d in range(1, n):
            o_copies[s, d].wait()
            numer = numer + factors[d] * o_recv[d, s].astype(f32)
        merged.append((numer / denom).astype(bf16))

    part = LATENT // nr
    for k in range(nr):
        for r in range(seqs * MTP):
            t = r % MTP
            a_send[k, r] = merged[r // MTP][t * heads:(t + 1) * heads, k * part:(k + 1) * part]
    copies = []
    for d in range(1, nr):
        k, device = fpeer(d)
        c = remote(a_send.at[k], out_ref.at[fme], sems.at[6 * seqs, d], sems.at[7 * seqs, d], device)
        c.start()
        copies.append(c)
    out_ref[fme] = a_send[fme]
    for d in range(1, nr):
        k, device = fpeer(nr - d)
        copies[d - 1].wait_send()
        remote(a_send.at[k], out_ref.at[k], sems.at[6 * seqs, d], sems.at[7 * seqs, d],
               device).wait_recv()


def layer_kernel(n, n_role, n_seq, q_ref, cache_hbm, len_ref, pos_ref, vu_hbm, res_ref, gain_ref,
                 wo_hbm, wg_hbm, wu_hbm, wd_hbm,
                 out_ref, cache, vu, q_all, o_send, o_recv, s_send, s_recv, a_send, a_all, a_head,
                 mixed, pv_ref, wo, wg, wu, wd, pv_recv, v_send, v_all, v_full, acc, po_send,
                 po_recv, resid, xg_ref, g_acc, u_acc, gu_send, gu_recv, ss_send, ss_recv, h_send,
                 h_all, h_full, dn, dn_send, dn_recv, wsem, lsem, asems, sems):
    nr = n_role * n_seq
    me, peer = ctx_group(n)
    fme, fpeer = feature_group(n_role, n_seq)

    cache_copy = pltpu.make_async_copy(cache_hbm, cache, lsem.at[0])
    cache_copy.start()
    vu_copy = pltpu.make_async_copy(vu_hbm, vu, lsem.at[1])
    vu_copy.start()
    weights = []
    for which, (hbm, vmem) in enumerate(((wo_hbm, wo), (wg_hbm, wg), (wu_hbm, wu), (wd_hbm, wd))):
        depth = vmem.shape[1]

        def fetch(i, hbm=hbm, vmem=vmem, depth=depth, which=which):
            return pltpu.make_async_copy(
                hbm.at[pl.ds(i * depth, depth)], vmem.at[i], wsem.at[which, i])

        weights.append((fetch, vmem))
    for fetch, vmem in weights:
        for i in range(vmem.shape[0]):
            fetch(i).start()
    enter(((n, peer), (nr, fpeer)))
    attend(n, n_role, n_seq, q_ref, cache, cache_copy, len_ref, pos_ref, a_all,
           q_all, o_send, o_recv, s_send, s_recv, a_send, asems)
    rows, heads = a_all.shape[1:3]
    for j in range(nr):
        for r in range(rows):
            a_head[:, j * rows + r, :] = a_all[j, r].astype(f32)
    vu_copy.wait()
    vdim = vu.shape[2]
    for h in range(heads):
        mixed[:, h * vdim:(h + 1) * vdim] = jnp.dot(
            a_head[h].astype(bf16), vu[h], preferred_element_type=f32)
    for k in range(nr):
        pv_ref[k] = mixed[k * rows:(k + 1) * rows, :].astype(bf16)

    def matmul(x_ref, *pairs):
        chunks, depth, _ = weights[pairs[0][0]][1].shape
        for which, acc_ref in pairs:
            fetch, vmem = weights[which]
            fetch(0).wait()
            acc_ref[...] = jnp.dot(x_ref[:, :depth], vmem[0], preferred_element_type=f32)
        if chunks == 1:
            return

        @pl.loop(1, chunks)
        def _(i):
            x = x_ref[:, pl.ds(pl.multiple_of(i * depth, depth), depth)]
            for which, acc_ref in pairs:
                fetch, vmem = weights[which]
                fetch(i).wait()
                acc_ref[...] += jnp.dot(x, vmem[i], preferred_element_type=f32)

    def swap(size, peer_of, chunk, recv, row):
        copies = []
        for d in range(1, size):
            k, device = peer_of(d)
            c = remote(chunk(k), recv.at[d], sems.at[row, d], sems.at[row + 1, d], device)
            c.start()
            copies.append(c)
        return copies

    def gather(size, my, peer_of, send, full, row):
        copies = []
        for d in range(1, size):
            c = remote(send, full.at[my], sems.at[row, d], sems.at[row + 1, d], peer_of(d)[1])
            c.start()
            copies.append(c)
        full[my] = send[...]
        for d in range(1, size):
            k, device = peer_of(size - d)
            copies[d - 1].wait_send()
            remote(send, full.at[k], sems.at[row, d], sems.at[row + 1, d], device).wait_recv()

    part = res_ref.shape[0] // nr
    copies = swap(nr, fpeer, lambda k: pv_ref.at[k], pv_recv, 0)
    vals = pv_ref[fme].astype(f32)
    for d in range(1, nr):
        copies[d - 1].wait()
        vals = vals + pv_recv[d].astype(f32)
    v_send[...] = vals.astype(bf16)
    gather(nr, fme, fpeer, v_send, v_all, 2)
    for k in range(nr):
        acc_rows = v_all[k].astype(f32)
        v_full[k * part:(k + 1) * part, :] = acc_rows
    x_ref = xg_ref[0]
    x_ref[...] = v_full[...].astype(bf16)
    matmul(x_ref, (0, acc))

    po_send[...] = acc[...].astype(bf16)
    copies = swap(n, peer, lambda k: po_send, po_recv, 4)
    total = res_ref[...].astype(f32) + acc[...]
    for d in range(1, n):
        copies[d - 1].wait()
        total = total + po_recv[d].astype(f32)
    crows = res_ref.shape[0] // n
    for k in range(n):
        resid[k] = total[k * crows:(k + 1) * crows]
    sumsq = jnp.sum(total * total, axis=1, keepdims=True)
    sumsq = jnp.broadcast_to(sumsq, (total.shape[0], 128))
    for k in range(nr):
        ss_send[k] = sumsq[k * part:(k + 1) * part]
    s_copies = swap(nr, fpeer, lambda k: ss_send.at[k], ss_recv, 6)
    x_ref = xg_ref[1]
    x_ref[...] = (total * gain_ref[...]).astype(bf16)
    matmul(x_ref, (1, g_acc), (2, u_acc))

    for j, a in enumerate((g_acc, u_acc)):
        for k in range(nr):
            gu_send[k, j] = a[k * part:(k + 1) * part, :].astype(bf16)
    copies = swap(nr, fpeer, lambda k: gu_send.at[k], gu_recv, 8)
    ss = ss_send[fme]
    for d in range(1, nr):
        s_copies[d - 1].wait()
        ss = ss + ss_recv[d]
    inv = lax.rsqrt(ss[:, 0:1] / D + epsilon)
    gate = gu_send[fme, 0].astype(f32)
    up = gu_send[fme, 1].astype(f32)
    for d in range(1, nr):
        copies[d - 1].wait()
        gate = gate + gu_recv[d, 0].astype(f32)
        up = up + gu_recv[d, 1].astype(f32)
    gate = gate * inv
    up = up * inv
    h_send[...] = (gate / (1.0 + jnp.exp(-gate)) * up).astype(bf16)
    gather(nr, fme, fpeer, h_send, h_all, 10)
    for k in range(nr):
        h_full[k * part:(k + 1) * part, :] = h_all[k].astype(f32)
    x_ref = xg_ref[2]
    x_ref[...] = h_full[...].astype(bf16)
    matmul(x_ref, (3, acc))

    for k in range(n):
        piece = acc[k * crows:(k + 1) * crows, :]
        dn[k] = piece
        dn_send[k] = piece.astype(bf16)
    copies = swap(n, peer, lambda k: dn_send.at[k], dn_recv, 12)
    result = resid[me] + dn[me]
    for d in range(1, n):
        copies[d - 1].wait()
        result = result + dn_recv[d].astype(f32)
    out_ref[...] = result.astype(bf16)


def chunk_of(depth):
    for size in (1024, 768, 512, 256):
        if depth % size == 0:
            return size
    return depth


def per_device(sizes, queries, cache, lengths, positions, value_up_weight, out_proj, residual,
               norm_gain, gate_weight, up_weight, down_weight):
    n, n_role, n_seq = sizes
    nr = n_role * n_seq
    rows, heads, width = queries.shape
    seqs = cache.shape[0]
    span = rows * heads // seqs
    lat = LATENT // nr
    vmem = pl.BlockSpec(memory_space=pltpu.VMEM)
    smem = pl.BlockSpec(memory_space=pltpu.SMEM)
    hbm = pl.BlockSpec(memory_space=pl.ANY)
    most = max(n, nr)
    sems = lambda k: pltpu.SemaphoreType.DMA((k, most))
    vwide = heads * value_up_weight.shape[2]
    all_rows, dd = residual.shape
    ff = gate_weight.shape[1]
    part, crows = all_rows // nr, all_rows // n

    def held(w):
        size = chunk_of(w.shape[0])
        return pltpu.VMEM((w.shape[0] // size, size, w.shape[1]), bf16)

    ws = (out_proj, gate_weight, up_weight, down_weight)
    most_chunks = max(w.shape[0] // chunk_of(w.shape[0]) for w in ws)
    V = pltpu.VMEM
    return pl.pallas_call(
        functools.partial(layer_kernel, n, n_role, n_seq),
        out_shape=jax.ShapeDtypeStruct((crows, dd), bf16),
        in_specs=[vmem, hbm, smem, smem, hbm, vmem, vmem] + [hbm] * 4,
        out_specs=vmem,
        scratch_shapes=[
            V((cache.shape[0], width, cache.shape[1]), bf16),
            V(value_up_weight.shape, bf16),
            V((n, seqs, span, width), bf16),
            V((n, seqs, span, LATENT), bf16),
            V((n, seqs, span, LATENT), bf16),
            V((n, seqs, 8, span), f32),
            V((n, seqs, 8, span), f32),
            V((nr, rows, heads, lat), bf16),
            V((nr, rows, heads, lat), bf16),
            V((heads, all_rows, lat), f32),
            V((all_rows, vwide), f32),
            V((nr, part, vwide), bf16),
            *[held(w) for w in ws],
            V((nr, part, vwide), bf16),
            V((part, vwide), bf16),
            V((nr, part, vwide), bf16),
            V((all_rows, vwide), f32),
            V((all_rows, dd), f32),
            V((all_rows, dd), bf16),
            V((n, all_rows, dd), bf16),
            V((n, crows, dd), f32),
            [V((all_rows, vwide), bf16), V((all_rows, dd), bf16), V((all_rows, ff), bf16)],
            V((all_rows, ff), f32),
            V((all_rows, ff), f32),
            V((nr, 2, part, ff), bf16),
            V((nr, 2, part, ff), bf16),
            V((nr, part, 128), f32),
            V((nr, part, 128), f32),
            V((part, ff), bf16),
            V((nr, part, ff), bf16),
            V((all_rows, ff), f32),
            V((n, crows, dd), f32),
            V((n, crows, dd), bf16),
            V((n, crows, dd), bf16),
            pltpu.SemaphoreType.DMA((4, most_chunks)),
            pltpu.SemaphoreType.DMA((2,)),
            sems(8 * seqs),
            sems(14),
        ],
        compiler_params=pltpu.CompilerParams(
            collective_id=0, has_side_effects=True, vmem_limit_bytes=VMEM_BYTES),
        name="layer",
    )(queries.reshape(seqs, span, width), cache.transpose(0, 2, 1), lengths, positions, value_up_weight,
      residual, norm_gain.reshape(1, dd), *ws)


def solution(mesh):
    placed = (
        P(("groups", "role", "seq"), "ctx", None),
        P(("groups", "role", "seq"), "ctx", None),
        P(("groups", "role", "seq")),
        P(("groups", "role", "seq")),
        P("ctx", ("role", "seq"), None),
        P("ctx", ("role", "seq")),
        P("groups", ("role", "seq")),
        P(("role", "seq")),
        P(("role", "seq"), "ctx"),
        P(("role", "seq"), "ctx"),
        P("ctx", ("role", "seq")),
    )
    sizes = (mesh.shape["ctx"], mesh.shape["role"], mesh.shape["seq"])
    return jax.shard_map(
        functools.partial(per_device, sizes),
        mesh=mesh,
        in_specs=placed,
        out_specs=P(("groups", "ctx"), ("role", "seq")),
        check_vma=False,
    )
```
